8 devices in a mesh: rep: 1 (over z), r: 2 (over y), s: 4 (over x, core).
Axes of the slice: x: 2, y: 2, z: 1, core: 2. Of those that a mesh axis runs over, the one named last changes fastest.
Arguments:
- x: bfloat16 [8, 4096, 1024], P(('rep', 'r', 's'))
- dy: bfloat16 [8, 4096, 1024], P(('rep', 'r', 's'))
- w_gate: bfloat16 [2, 1024, 2816], P(None, 's')
- w_up: bfloat16 [2, 1024, 2816], P(None, 's')
- w_down: bfloat16 [2, 2816, 1024], P(None, 's')
Outputs:
- output 1: bfloat16 [8, 4096, 1024], P(('rep', 'r', 's'))
- output 2: bfloat16 [2, 1024, 2816], P('rep', 's')
- output 3: bfloat16 [2, 1024, 2816], P('rep', 's')
- output 4: bfloat16 [2, 2816, 1024], P('rep', 's')
All inputs are finite; a program needn't handle non-finite values.
Results may differ from the reference program's by a relative error of at most 0.018.
Values are sent between devices in bfloat16 or wider.
A program may use at most 2 GiB of HBM per device.

```python
import jax
import jax.numpy as jnp
from jax import lax

SEQUENCES = 8
TOKENS = 4096
D = 1024
FF = 2816
LAYERS = 2
NAMES = ("w_gate", "w_up", "w_down")
SHAPES = {"w_gate": (LAYERS, D, FF), "w_up": (LAYERS, D, FF), "w_down": (LAYERS, FF, D)}


def bump(key, n, height):
    away = (jnp.arange(n, dtype=jnp.int32) - jax.random.randint(key, (), 0, n, jnp.int32)) % n
    return jnp.where(away < n // 8, height, 1.0)


def together(key, own, strength):
    shared = jax.random.normal(key, own.shape[1:], jnp.float32)
    return (own + strength * shared) * lax.rsqrt(1 + strength * strength)


def setup_inputs(seed: int = 0, part: int = 0) -> dict:
    kx, kdy, ka, kb, kz, kf, kh, kl, *kw = jax.random.split(jax.random.key(seed), 8 + len(NAMES))
    kx, kdy, ka, kb = (jax.random.fold_in(k, part) for k in (kx, kdy, ka, kb))
    shape = (SEQUENCES, TOKENS, D)
    much_x, much_dy = jax.random.uniform(kz, (2,), jnp.float32, 0.0, 1.0)
    layers = 2.0 ** jax.random.uniform(kl, (LAYERS, 1, 1), jnp.float32, -1.0, 1.0)
    x = together(ka, jax.random.normal(kx, shape, jnp.float32), much_x) * bump(kf, D, 4.0)
    dy = together(kb, jax.random.normal(kdy, shape, jnp.float32), much_dy)
    drawn = {"x": x.astype(jnp.bfloat16), "dy": (dy * (SEQUENCES * TOKENS) ** -0.5).astype(jnp.bfloat16)}
    for key, name in zip(kw, NAMES, strict=True):
        w = jax.random.normal(key, SHAPES[name], jnp.float32) * SHAPES[name][1] ** -0.5
        drawn[name] = (w * {"w_gate": 1.0, "w_up": bump(kh, FF, 4.0), "w_down": layers}[name]).astype(jnp.bfloat16)
    return drawn


def matmul(a, w):
    return jnp.dot(a, w, preferred_element_type=jnp.float32).astype(jnp.bfloat16)


def normed(h):
    wide = h.astype(jnp.float32)
    scale = lax.rsqrt(jnp.mean(wide**2, -1, keepdims=True) + 1e-6)
    return (wide * scale).astype(jnp.bfloat16)


def layer(h, w):
    a = normed(h)
    gate = jnp.dot(a, w["w_gate"], preferred_element_type=jnp.float32)
    up = jnp.dot(a, w["w_up"], preferred_element_type=jnp.float32)
    return h + matmul((jax.nn.silu(gate) * up).astype(jnp.bfloat16), w["w_down"])


def stack(weights, h):
    return lax.scan(lambda h, w: (layer(h, w), None), h, weights)[0]


def reference(x, dy, w_gate, w_up, w_down):
    weights = dict(zip(NAMES, (w_gate, w_up, w_down), strict=True))

    def take(so_far, sequence):
        h, by_y = sequence
        _, back = jax.vjp(stack, weights, h)
        by_weights, by_h = back(by_y)
        return jax.tree.map(lambda total, term: total + term.astype(jnp.float32), so_far, by_weights), by_h

    none_yet = {name: jnp.zeros(w.shape, jnp.float32) for name, w in weights.items()}
    by_weights, by_x = lax.scan(take, none_yet, (x, dy))
    return (by_x, *(by_weights[name].astype(jnp.bfloat16) for name in NAMES))
```

```python
import functools

import jax
import jax.numpy as jnp
from jax import lax
from jax.experimental import pallas as pl
from jax.experimental.pallas import tpu as pltpu
from jax.sharding import PartitionSpec as P

F32, BF16 = jnp.float32, jnp.bfloat16
ROWS = 512
COLS = 256
VMEM_LIMIT = 60 * 1024 * 1024


def whole(shape):
    return pl.BlockSpec(shape, lambda i: (0,) * len(shape), pipeline_mode=pl.Buffered(1))


def tiles(rows, width):
    return pl.BlockSpec((rows, width), lambda i: (i, 0))


def columns(height, cols):
    return pl.BlockSpec((height, cols), lambda i: (0, i))


def params():
    return pltpu.CompilerParams(vmem_limit_bytes=VMEM_LIMIT, dimension_semantics=("arbitrary",))


def cost(matmuls, m, k, n, nbytes, exps=0):
    return pl.CostEstimate(flops=2 * matmuls * m * k * n, bytes_accessed=nbytes, transcendentals=exps)


def dot(a, b):
    return jnp.dot(a, b, preferred_element_type=F32)


def dot_nt(a, b):
    return lax.dot_general(a, b, (((1,), (1,)), ((), ())), preferred_element_type=F32)


def scale_of(wide):
    return lax.rsqrt(jnp.mean(wide * wide, -1, keepdims=True) + 1e-6)


def normed(h):
    wide = h.astype(F32)
    return (wide * scale_of(wide)).astype(BF16)


def hidden_kernel(h_ref, wg_ref, wu_ref, hidden_ref, gate_ref, a_ref):
    a_ref[...] = normed(h_ref[...])
    for c in range(wg_ref.shape[1] // COLS):
        at = slice(c * COLS, (c + 1) * COLS)
        gate = dot(a_ref[...], wg_ref[:, at])
        up = dot(a_ref[...], wu_ref[:, at])
        gate_ref[:, at] = gate
        hidden_ref[:, at] = (gate * jax.nn.sigmoid(gate) * up).astype(BF16)


def hidden_of(h, wg, wu):
    m, d = h.shape
    f = wg.shape[1]
    return pl.pallas_call(
        hidden_kernel,
        grid=(m // ROWS,),
        in_specs=[tiles(ROWS, d), whole((d, f)), whole((d, f))],
        out_specs=[tiles(ROWS, f), tiles(ROWS, f)],
        out_shape=[jax.ShapeDtypeStruct((m, f), BF16), jax.ShapeDtypeStruct((m, f), F32)],
        scratch_shapes=[pltpu.VMEM((ROWS, d), BF16)],
        compiler_params=params(),
        cost_estimate=cost(2, m, d, f, 2 * m * d + 4 * d * f + 6 * m * f, m * f),
        name="hidden",
    )(h, wg, wu)


def down_kernel(hidden_ref, wd_ref, h_ref, out_ref):
    for c in range(wd_ref.shape[1] // COLS):
        at = slice(c * COLS, (c + 1) * COLS)
        out_ref[:, at] = h_ref[:, at] + dot(hidden_ref[...], wd_ref[:, at]).astype(BF16)


def down_of(hidden, wd, h):
    m, d = h.shape
    f = wd.shape[0]
    return pl.pallas_call(
        down_kernel,
        grid=(m // ROWS,),
        in_specs=[tiles(ROWS, f), whole((f, d)), tiles(ROWS, d)],
        out_specs=tiles(ROWS, d),
        out_shape=jax.ShapeDtypeStruct((m, d), BF16),
        compiler_params=params(),
        cost_estimate=cost(1, m, d, f, 4 * m * d + 2 * d * f + 2 * m * f),
        name="down",
    )(hidden, wd, h)


def inner_kernel(kept, *refs):
    if kept:
        h_ref, g_ref, gate_ref, wu_ref, wd_ref, a_t_ref, hidden_t_ref, dgate_ref, dup_ref, a_ref = refs
    else:
        h_ref, g_ref, wg_ref, wu_ref, wd_ref, a_t_ref, hidden_t_ref, dgate_ref, dup_ref, a_ref = refs
    a = normed(h_ref[...])
    a_ref[...] = a
    a_t_ref[...] = a.T
    for c in range(wu_ref.shape[1] // COLS):
        at = slice(c * COLS, (c + 1) * COLS)
        gate = gate_ref[:, at] if kept else dot(a_ref[...], wg_ref[:, at])
        up = dot(a_ref[...], wu_ref[:, at])
        dhidden = dot_nt(g_ref[...], wd_ref[at, :]).astype(BF16).astype(F32)
        sig = jax.nn.sigmoid(gate)
        silu = gate * sig
        hidden_t_ref[at, :] = (silu * up).astype(BF16).T
        dup_ref[:, at] = (dhidden * silu).astype(BF16)
        dgate_ref[:, at] = (dhidden * up * (sig + silu * (1.0 - sig))).astype(BF16)


def inner_of(h, g, gate_or_wg, wu, wd, kept):
    m, d = h.shape
    f = wu.shape[1]
    return pl.pallas_call(
        functools.partial(inner_kernel, kept),
        grid=(m // ROWS,),
        in_specs=[
            tiles(ROWS, d),
            tiles(ROWS, d),
            tiles(ROWS, f) if kept else whole((d, f)),
            whole((d, f)),
            whole((f, d)),
        ],
        out_specs=[columns(d, ROWS), columns(f, ROWS), tiles(ROWS, f), tiles(ROWS, f)],
        out_shape=[
            jax.ShapeDtypeStruct((d, m), BF16),
            jax.ShapeDtypeStruct((f, m), BF16),
            jax.ShapeDtypeStruct((m, f), BF16),
            jax.ShapeDtypeStruct((m, f), BF16),
        ],
        scratch_shapes=[pltpu.VMEM((ROWS, d), BF16)],
        compiler_params=params(),
        cost_estimate=cost(2 if kept else 3, m, d, f, 6 * m * d + 6 * d * f + (10 if kept else 6) * m * f, m * f),
        name="inner_kept" if kept else "inner",
    )(h, g, gate_or_wg, wu, wd)


def outer_kernel(dgate_ref, dup_ref, wg_ref, wu_ref, h_ref, g_ref, out_ref, da_ref):
    for c in range(wg_ref.shape[0] // COLS):
        at = slice(c * COLS, (c + 1) * COLS)
        one = dot_nt(dgate_ref[...], wg_ref[at, :]).astype(BF16)
        two = dot_nt(dup_ref[...], wu_ref[at, :]).astype(BF16)
        da_ref[:, at] = one + two
    wide = h_ref[...].astype(F32)
    da = da_ref[...].astype(F32)
    scale = scale_of(wide)
    along = jnp.mean(da * wide, -1, keepdims=True)
    out_ref[...] = g_ref[...] + (scale * (da - wide * (along * scale * scale))).astype(BF16)


def outer_of(dgate, dup, wg, wu, h, g):
    m, d = h.shape
    f = wg.shape[1]
    return pl.pallas_call(
        outer_kernel,
        grid=(m // ROWS,),
        in_specs=[tiles(ROWS, f), tiles(ROWS, f), whole((d, f)), whole((d, f)), tiles(ROWS, d), tiles(ROWS, d)],
        out_specs=tiles(ROWS, d),
        out_shape=jax.ShapeDtypeStruct((m, d), BF16),
        scratch_shapes=[pltpu.VMEM((ROWS, d), BF16)],
        compiler_params=params(),
        cost_estimate=cost(2, m, d, f, 6 * m * d + 4 * d * f + 4 * m * f),
        name="outer",
    )(dgate, dup, wg, wu, h, g)


def by_columns_kernel(a_ref, b_ref, out_ref):
    out_ref[...] = dot(a_ref[...], b_ref[...]).astype(BF16)


def by_columns(a_t, b):
    d, m = a_t.shape
    f = b.shape[1]
    return pl.pallas_call(
        by_columns_kernel,
        grid=(f // COLS,),
        in_specs=[whole((d, m)), columns(m, COLS)],
        out_specs=columns(d, COLS),
        out_shape=jax.ShapeDtypeStruct((d, f), BF16),
        compiler_params=params(),
        cost_estimate=cost(1, m, d, f, 2 * m * d + 2 * d * f + 2 * m * f),
        name="by_columns",
    )(a_t, b)


def by_rows_kernel(a_ref, b_ref, out_ref):
    for c in range(b_ref.shape[1] // COLS):
        at = slice(c * COLS, (c + 1) * COLS)
        out_ref[:, at] = dot(a_ref[...], b_ref[:, at]).astype(BF16)


def by_rows(a_t, b):
    f, m = a_t.shape
    d = b.shape[1]
    rows = f // 4
    return pl.pallas_call(
        by_rows_kernel,
        grid=(4,),
        in_specs=[tiles(rows, m), whole((m, d))],
        out_specs=tiles(rows, d),
        out_shape=jax.ShapeDtypeStruct((f, d), BF16),
        compiler_params=params(),
        cost_estimate=cost(1, m, d, f, 2 * m * d + 2 * d * f + 2 * m * f),
        name="by_rows",
    )(a_t, b)


def solution(mesh):
    groups = mesh.shape["r"]
    other = [(i, (i + 1) % groups) for i in range(groups)]

    def fetched(w, number):
        return lax.all_gather(w[number], "s", axis=0, tiled=True)

    def summed(term):
        mine = lax.psum_scatter(term, "s", scatter_dimension=0, tiled=True)
        return mine.astype(F32) + lax.ppermute(mine, "r", other).astype(F32)

    def step(x, dy, w_gate, w_up, w_down):
        h0, g2 = x[0], dy[0]
        wg0, wu0, wd0 = (fetched(w, 0) for w in (w_gate, w_up, w_down))
        wg1, wu1, wd1 = (fetched(w, 1) for w in (w_gate, w_up, w_down))
        hidden, gate = hidden_of(h0, wg0, wu0)
        h1 = down_of(hidden, wd0, h0)

        a_t, hidden_t, dgate, dup = inner_of(h1, g2, wg1, wu1, wd1, False)
        down1 = summed(by_rows(hidden_t, g2))
        gate1 = summed(by_columns(a_t, dgate))
        up1 = summed(by_columns(a_t, dup))
        g1 = outer_of(dgate, dup, wg1, wu1, h1, g2)

        a_t, hidden_t, dgate, dup = inner_of(h0, g1, gate, wu0, wd0, True)
        down0 = summed(by_rows(hidden_t, g1))
        gate0 = summed(by_columns(a_t, dgate))
        up0 = summed(by_columns(a_t, dup))
        g0 = outer_of(dgate, dup, wg0, wu0, h0, g1)
        pairs = ((gate0, gate1), (up0, up1), (down0, down1))
        return (g0[None], *(jnp.stack(pair).astype(BF16) for pair in pairs))

    states, cut = P(("rep", "r", "s"), None, None), P(None, "s", None)
    return jax.shard_map(
        step,
        mesh=mesh,
        in_specs=(states, states) + (cut,) * 3,
        out_specs=(states,) + (P("rep", "s", None),) * 3,
        check_vma=False,
    )
```

```python
import functools

import jax
import jax.numpy as jnp
from jax import lax
from jax.experimental import pallas as pl
from jax.experimental.pallas import tpu as pltpu
from jax.sharding import PartitionSpec as P

F32, BF16 = jnp.float32, jnp.bfloat16
ROWS = 512
COLS = 256
VMEM_LIMIT = 60 * 1024 * 1024


def whole(shape):
    return pl.BlockSpec(shape, lambda i: (0,) * len(shape), pipeline_mode=pl.Buffered(1))


def tiles(rows, width):
    return pl.BlockSpec((rows, width), lambda i: (i, 0))


def columns(height, cols):
    return pl.BlockSpec((height, cols), lambda i: (0, i))


def ordered(kernel, inputs, after):
    return (lambda *refs: kernel(*refs[:inputs], *refs[inputs + len(after) :])), [pl.BlockSpec(memory_space=pl.ANY)] * len(after)


def params():
    return pltpu.CompilerParams(vmem_limit_bytes=VMEM_LIMIT, dimension_semantics=("arbitrary",))


def cost(matmuls, m, k, n, nbytes, exps=0):
    return pl.CostEstimate(flops=2 * matmuls * m * k * n, bytes_accessed=nbytes, transcendentals=exps)


def dot(a, b):
    return jnp.dot(a, b, preferred_element_type=F32)


def dot_nt(a, b):
    return lax.dot_general(a, b, (((1,), (1,)), ((), ())), preferred_element_type=F32)


def scale_of(wide):
    return lax.rsqrt(jnp.mean(wide * wide, -1, keepdims=True) + 1e-6)


def normed(h):
    wide = h.astype(F32)
    return (wide * scale_of(wide)).astype(BF16)


FEW = 2
LEAD = 2


def forward_kernel(
    h_ref, wg_ref, wu_ref, wd_ref,
    wg0_ref, wu0_ref, wd0_ref, wg1_ref, wu1_ref, wd1_ref, hidden_ref, gate_ref, out_ref,
    a_ref, wg_all, wu_all, wd_all, hidden_out, gate_out, hidden_in, h_in, h_out,
    send, recv, send_b, recv_b, send_own, recv_own, local, load, store,
):
    r, s = lax.axis_index("r"), lax.axis_index("s")
    sibling, across = lax.rem(s, 2), lax.rem(s + 2, 4)
    sibling = s + 1 - 2 * sibling
    m, d = h_ref.shape
    f = wg_all.shape[1]
    steps = f // COLS
    shard, shard_d = wg_ref.shape[1], wd_ref.shape[1]
    half, half_d = shard // 2, shard_d // 2

    def remote(src, dst, sends, recvs, where):
        return pltpu.make_async_remote_copy(
            src_ref=src, dst_ref=dst, send_sem=sends, recv_sem=recvs, device_id=where, device_id_type=pl.DeviceIdType.MESH
        )

    def hop(kind, own, whole_ref, size, row, rows, at, sends, recvs):
        part = size // 2
        if kind == 1:
            first = r * part + row
            return remote(
                own.at[pl.ds(first, rows), at],
                whole_ref.at[pl.ds(s * size + first, rows), at],
                sends, recvs, {"s": across},
            )
        which = r if kind < 4 else 1 - r
        there = whole_ref.at[pl.ds(across * size + which * part + row, rows), at]
        return remote(there, there, sends, recvs, {"r": 1 - r} if kind == 3 else {"s": sibling})

    def fine(kind, which, n):
        own, every = ((wg_ref, wg_all), (wu_ref, wu_all))[which]
        at = pl.ds(pl.multiple_of(n * COLS, COLS), COLS)
        if kind == 0:
            return remote(
                own.at[0, :, at], every.at[pl.ds(pl.multiple_of(s * shard, shard), shard), at],
                send.at[n, which, 0], recv.at[n, which, 0], {"s": sibling},
            )
        return hop(kind, own.at[0], every, shard, 0, half, at, send.at[n, which, kind], recv.at[n, which, kind])

    behind = ((wd_ref, 0, wd_all), (wg_ref, 1, wg1_ref), (wu_ref, 1, wu1_ref), (wd_ref, 1, wd1_ref))

    def coarse(kind, which, piece):
        own, number, every = behind[which]
        size = own.shape[1]
        rows = size // 2 // FEW
        return hop(
            kind, own.at[number], every, size, piece * rows, rows, slice(None),
            send_b.at[which, piece, kind - 1], recv_b.at[which, piece, kind - 1],
        )

    def coarse_own(which):
        own, number, every = behind[which]
        size = own.shape[1]
        return remote(own.at[number], every.at[pl.ds(s * size, size)], send_own.at[which], recv_own.at[which], {"s": sibling})

    def place_own(which):
        own, number, every = ((wg_ref, 0, wg_all), (wu_ref, 0, wu_all), *behind)[which]
        size = own.shape[1]
        return pltpu.make_async_copy(own.at[number], every.at[pl.ds(s * size, size)], local.at[which])

    load_h = pltpu.make_async_copy(h_ref, a_ref, load.at[0])
    load_h.start()
    for which in range(2):
        place_own(which).start()

    def first_sends(n, carry):
        for which in range(2):
            fine(1, which, n).start()
        return carry

    def own_sends(n):
        for which in range(2):
            fine(0, which, n).start()

    first_sends(0, 0)
    own_sends(0)
    own_sends(1)
    lax.fori_loop(1, steps, first_sends, 0)

    def send_on(n):
        for which in range(2):
            fine(1, which, n).wait_recv()
            fine(2, which, n).start()
            fine(3, which, n).start()

    def send_last(n):
        for which in range(2):
            fine(3, which, n).wait_recv()
            fine(4, which, n).start()

    load_h.wait()
    for row in range(0, m, ROWS):
        a_ref[row : row + ROWS, :] = normed(a_ref[row : row + ROWS, :])
    send_on(0)
    send_on(1)
    send_last(0)
    place_own(0).wait()
    place_own(1).wait()

    def out_copies(n):
        slot = lax.rem(n, 2)
        at = pl.ds(pl.multiple_of(n * COLS, COLS), COLS)
        return (
            pltpu.make_async_copy(hidden_out.at[slot], hidden_ref.at[:, at], store.at[0, slot]),
            pltpu.make_async_copy(gate_out.at[slot], gate_ref.at[:, at], store.at[1, slot]),
        )

    def coarse_on(which, piece):
        coarse(1, which, piece).wait_recv()
        coarse(2, which, piece).start()
        coarse(3, which, piece).start()

    def coarse_last(which, piece):
        coarse(3, which, piece).wait_recv()
        coarse(4, which, piece).start()

    def begin(which):
        place_own(2 + which).start()
        coarse_own(which).start()
        for piece in range(FEW):
            coarse(1, which, piece).start()

    def step(n, carry):
        @pl.when(n >= 2)
        def _():
            for copy in out_copies(n - 2):
                copy.wait()

        @pl.when(n + 2 < steps)
        def _():
            own_sends(n + 2)
            send_on(n + 2)

        for which in range(4):
            @pl.when(n == 2 * which + 1)
            def _(which=which):
                begin(which)

        for number, at_step in enumerate((6, 8, 9, 10)):
            @pl.when(n == at_step)
            def _(number=number):
                coarse_on(number // FEW, number % FEW)

        for which in range(2):
            for kind in (0, 2, 4):
                fine(kind, which, n).wait_recv()
        slot = lax.rem(n, 2)
        at = pl.ds(pl.multiple_of(n * COLS, COLS), COLS)
        def block(row):
            rows = slice(row, row + 1024)
            gate = dot(a_ref[rows, :], wg_all[:, at])
            up = dot(a_ref[rows, :], wu_all[:, at])
            gate_out[slot, rows, :] = gate
            hidden_out[slot, rows, :] = (gate * jax.nn.sigmoid(gate) * up).astype(BF16)

        block(0)
        block(1024)

        @pl.when(n + 1 < steps)
        def _():
            send_last(n + 1)

        block(2048)
        block(3072)
        for copy in out_copies(n):
            copy.start()
        return carry

    lax.fori_loop(0, steps, step, 0)

    def tile_loads(i):
        slot = lax.rem(i, 2)
        rows = pl.ds(pl.multiple_of(i * ROWS, ROWS), ROWS)
        return (
            pltpu.make_async_copy(hidden_ref.at[rows], hidden_in.at[slot], load.at[slot]),
            pltpu.make_async_copy(h_ref.at[rows], h_in.at[slot], load.at[2 + slot]),
        )

    def tile_store(i):
        slot = lax.rem(i, 2)
        rows = pl.ds(pl.multiple_of(i * ROWS, ROWS), ROWS)
        return pltpu.make_async_copy(h_out.at[slot], out_ref.at[rows], store.at[2, slot])

    for piece in range(FEW):
        coarse_last(0, piece)
    saves = [
        pltpu.make_async_copy(every, kept, local.at[which])
        for which, (every, kept) in enumerate(((wg_all, wg0_ref), (wu_all, wu0_ref)))
    ]
    for save in saves:
        save.start()
    for n in (steps - 2, steps - 1):
        for copy in out_copies(n):
            copy.wait()
    for copy in tile_loads(0):
        copy.start()
    place_own(2).wait()
    coarse_own(0).wait_recv()
    for piece in range(FEW):
        coarse(2, 0, piece).wait_recv()
        coarse(4, 0, piece).wait_recv()
    save_down = pltpu.make_async_copy(wd_all, wd0_ref, local.at[2])
    save_down.start()
    tile_count = m // ROWS

    def tile(i, carry):
        @pl.when(i + 1 < tile_count)
        def _():
            for copy in tile_loads(i + 1):
                copy.start()

        @pl.when(i >= 2)
        def _():
            tile_store(i - 2).wait()

        for at_tile, number in ((1, 4), (3, 5), (5, 6), (7, 7)):
            @pl.when(i == at_tile)
            def _(number=number):
                coarse_on(number // FEW, number % FEW)

        for at_tile, number in ((0, 2), (2, 3), (4, 4), (6, 5)):
            @pl.when(i == at_tile)
            def _(number=number):
                coarse_last(number // FEW, number % FEW)

        for copy in tile_loads(i):
            copy.wait()
        slot = lax.rem(i, 2)
        for c in range(d // COLS):
            at = slice(c * COLS, (c + 1) * COLS)
            h_out[slot, :, at] = h_in[slot, :, at] + dot(hidden_in[slot], wd_all[:, at]).astype(BF16)
        tile_store(i).start()
        return carry

    lax.fori_loop(0, tile_count, tile, 0)
    for piece in range(FEW):
        coarse_last(3, piece)
    for i in (tile_count - 2, tile_count - 1):
        tile_store(i).wait()
    for save in (*saves, save_down):
        save.wait()
    for which in range(1, 4):
        place_own(2 + which).wait()
        coarse_own(which).wait_recv()
        for piece in range(FEW):
            coarse(2, which, piece).wait_recv()
            coarse(4, which, piece).wait_recv()
    for which in range(4):
        coarse_own(which).wait_send()
        for piece in range(FEW):
            for kind in range(1, 5):
                coarse(kind, which, piece).wait_send()

    def finish(n, carry):
        for which in range(2):
            for kind in range(5):
                fine(kind, which, n).wait_send()
        return carry

    lax.fori_loop(0, steps, finish, 0)


def forward(h, w_gate, w_up, w_down):
    m, d = h.shape
    f = w_gate.shape[2]
    steps = f // COLS
    any_spec = pl.BlockSpec(memory_space=pl.ANY)
    up_shape, down_shape = jax.ShapeDtypeStruct((d, f), BF16), jax.ShapeDtypeStruct((f, d), BF16)
    dma = pltpu.SemaphoreType.DMA
    return pl.pallas_call(
        forward_kernel,
        in_specs=[any_spec] * 4,
        out_specs=[any_spec] * 9,
        out_shape=[
            up_shape, up_shape, down_shape, up_shape, up_shape, down_shape,
            jax.ShapeDtypeStruct((m, f), BF16),
            jax.ShapeDtypeStruct((m, f), F32),
            jax.ShapeDtypeStruct((m, d), BF16),
        ],
        scratch_shapes=[
            pltpu.VMEM((m, d), BF16),
            pltpu.VMEM((d, f), BF16),
            pltpu.VMEM((d, f), BF16),
            pltpu.VMEM((f, d), BF16),
            pltpu.VMEM((2, m, COLS), BF16),
            pltpu.VMEM((2, m, COLS), F32),
            pltpu.VMEM((2, ROWS, f), BF16),
            pltpu.VMEM((2, ROWS, d), BF16),
            pltpu.VMEM((2, ROWS, d), BF16),
            dma((steps, 2, 5)), dma((steps, 2, 5)),
            dma((4, FEW, 4)), dma((4, FEW, 4)),
            dma((4,)), dma((4,)), dma((6,)), dma((4,)), dma((3, 2)),
        ],
        compiler_params=pltpu.CompilerParams(vmem_limit_bytes=VMEM_LIMIT, has_side_effects=True),
        cost_estimate=cost(3, m, d, f, 4 * m * d + 24 * d * f + 8 * m * f, m * f),
        name="forward",
    )(h, w_gate, w_up, w_down)


def inner_kernel(kept, *refs):
    if kept:
        h_ref, g_ref, gate_ref, wu_ref, wd_ref, a_t_ref, hidden_t_ref, dgate_ref, dup_ref, a_ref = refs
    else:
        h_ref, g_ref, wg_ref, wu_ref, wd_ref, a_t_ref, hidden_t_ref, dgate_ref, dup_ref, a_ref = refs
    a = normed(h_ref[...])
    a_ref[...] = a
    a_t_ref[...] = a.T
    for c in range(wu_ref.shape[1] // COLS):
        at = slice(c * COLS, (c + 1) * COLS)
        gate = gate_ref[:, at] if kept else dot(a_ref[...], wg_ref[:, at])
        up = dot(a_ref[...], wu_ref[:, at])
        dhidden = dot_nt(g_ref[...], wd_ref[at, :]).astype(BF16).astype(F32)
        sig = jax.nn.sigmoid(gate)
        silu = gate * sig
        hidden_t_ref[at, :] = (silu * up).astype(BF16).T
        dup_ref[:, at] = (dhidden * silu).astype(BF16)
        dgate_ref[:, at] = (dhidden * up * (sig + silu * (1.0 - sig))).astype(BF16)


def inner_of(h, g, gate_or_wg, wu, wd, kept, after=()):
    m, d = h.shape
    f = wu.shape[1]
    kernel, extra = ordered(functools.partial(inner_kernel, kept), 5, after)
    return pl.pallas_call(
        kernel,
        grid=(m // ROWS,),
        in_specs=[
            tiles(ROWS, d),
            tiles(ROWS, d),
            tiles(ROWS, f) if kept else whole((d, f)),
            whole((d, f)),
            whole((f, d)),
            *extra,
        ],
        out_specs=[columns(d, ROWS), columns(f, ROWS), tiles(ROWS, f), tiles(ROWS, f)],
        out_shape=[
            jax.ShapeDtypeStruct((d, m), BF16),
            jax.ShapeDtypeStruct((f, m), BF16),
            jax.ShapeDtypeStruct((m, f), BF16),
            jax.ShapeDtypeStruct((m, f), BF16),
        ],
        scratch_shapes=[pltpu.VMEM((ROWS, d), BF16)],
        compiler_params=params(),
        cost_estimate=cost(2 if kept else 3, m, d, f, 6 * m * d + 6 * d * f + (10 if kept else 6) * m * f, m * f),
        name="inner_kept" if kept else "inner",
    )(h, g, gate_or_wg, wu, wd, *after)


def outer_kernel(dgate_ref, dup_ref, wg_ref, wu_ref, h_ref, g_ref, out_ref, da_ref):
    for c in range(wg_ref.shape[0] // COLS):
        at = slice(c * COLS, (c + 1) * COLS)
        one = dot_nt(dgate_ref[...], wg_ref[at, :]).astype(BF16)
        two = dot_nt(dup_ref[...], wu_ref[at, :]).astype(BF16)
        da_ref[:, at] = one + two
    wide = h_ref[...].astype(F32)
    da = da_ref[...].astype(F32)
    scale = scale_of(wide)
    along = jnp.mean(da * wide, -1, keepdims=True)
    out_ref[...] = g_ref[...] + (scale * (da - wide * (along * scale * scale))).astype(BF16)


def outer_of(dgate, dup, wg, wu, h, g, after=()):
    m, d = h.shape
    f = wg.shape[1]
    kernel, extra = ordered(outer_kernel, 6, after)
    return pl.pallas_call(
        kernel,
        grid=(m // ROWS,),
        in_specs=[tiles(ROWS, f), tiles(ROWS, f), whole((d, f)), whole((d, f)), tiles(ROWS, d), tiles(ROWS, d), *extra],
        out_specs=tiles(ROWS, d),
        out_shape=jax.ShapeDtypeStruct((m, d), BF16),
        scratch_shapes=[pltpu.VMEM((ROWS, d), BF16)],
        compiler_params=params(),
        cost_estimate=cost(2, m, d, f, 6 * m * d + 4 * d * f + 4 * m * f),
        name="outer",
    )(dgate, dup, wg, wu, h, g, *after)


def by_columns_kernel(a_ref, b_ref, out_ref):
    out_ref[...] = dot(a_ref[...], b_ref[...]).astype(BF16)


def by_columns(a_t, b, after=()):
    d, m = a_t.shape
    f = b.shape[1]
    kernel, extra = ordered(by_columns_kernel, 2, after)
    return pl.pallas_call(
        kernel,
        grid=(f // COLS,),
        in_specs=[whole((d, m)), columns(m, COLS), *extra],
        out_specs=columns(d, COLS),
        out_shape=jax.ShapeDtypeStruct((d, f), BF16),
        compiler_params=params(),
        cost_estimate=cost(1, m, d, f, 2 * m * d + 2 * d * f + 2 * m * f),
        name="by_columns",
    )(a_t, b, *after)


def by_rows_kernel(a_ref, b_ref, out_ref):
    for c in range(b_ref.shape[1] // COLS):
        at = slice(c * COLS, (c + 1) * COLS)
        out_ref[:, at] = dot(a_ref[...], b_ref[:, at]).astype(BF16)


def by_rows(a_t, b, after=()):
    f, m = a_t.shape
    d = b.shape[1]
    rows = f // 4
    kernel, extra = ordered(by_rows_kernel, 2, after)
    return pl.pallas_call(
        kernel,
        grid=(4,),
        in_specs=[tiles(rows, m), whole((m, d)), *extra],
        out_specs=tiles(rows, d),
        out_shape=jax.ShapeDtypeStruct((f, d), BF16),
        compiler_params=params(),
        cost_estimate=cost(1, m, d, f, 2 * m * d + 2 * d * f + 2 * m * f),
        name="by_rows",
    )(a_t, b, *after)


def solution(mesh):
    groups = mesh.shape["r"]
    other = [(i, (i + 1) % groups) for i in range(groups)]

    def summed(term):
        mine = lax.psum_scatter(term, "s", scatter_dimension=0, tiled=True)
        return mine.astype(F32) + lax.ppermute(mine, "r", other).astype(F32)

    def step(x, dy, w_gate, w_up, w_down):
        h0, g2 = x[0], dy[0]
        wg0, wu0, wd0, wg1, wu1, wd1, _, gate, h1 = forward(h0, w_gate, w_up, w_down)

        a_t, hidden_t, dgate, dup = inner_of(h1, g2, wg1, wu1, wd1, False)
        by_down = by_rows(hidden_t, g2)
        by_gate = by_columns(a_t, dgate, (by_down,))
        by_up = by_columns(a_t, dup, (by_gate,))
        down1, gate1, up1 = summed(by_down), summed(by_gate), summed(by_up)
        g1 = outer_of(dgate, dup, wg1, wu1, h1, g2, (by_up,))

        a_t, hidden_t, dgate, dup = inner_of(h0, g1, gate, wu0, wd0, True)
        by_down = by_rows(hidden_t, g1)
        by_gate = by_columns(a_t, dgate, (by_down,))
        by_up = by_columns(a_t, dup, (by_gate,))
        down0, gate0, up0 = summed(by_down), summed(by_gate), summed(by_up)
        g0 = outer_of(dgate, dup, wg0, wu0, h0, g1, (by_up,))
        pairs = ((gate0, gate1), (up0, up1), (down0, down1))
        return (g0[None], *(jnp.stack(pair).astype(BF16) for pair in pairs))

    states, cut = P(("rep", "r", "s"), None, None), P(None, "s", None)
    return jax.shard_map(
        step,
        mesh=mesh,
        in_specs=(states, states) + (cut,) * 3,
        out_specs=(states,) + (P("rep", "s", None),) * 3,
        check_vma=False,
    )
```

```python
import functools

import jax
import jax.numpy as jnp
from jax import lax
from jax.experimental import pallas as pl
from jax.experimental.pallas import tpu as pltpu
from jax.sharding import PartitionSpec as P

F32, BF16 = jnp.float32, jnp.bfloat16
ROWS = 512
COLS = 256
VMEM_LIMIT = 60 * 1024 * 1024


def whole(shape):
    return pl.BlockSpec(shape, lambda i: (0,) * len(shape), pipeline_mode=pl.Buffered(1))


def tiles(rows, width):
    return pl.BlockSpec((rows, width), lambda i: (i, 0))


def columns(height, cols):
    return pl.BlockSpec((height, cols), lambda i: (0, i))


def ordered(kernel, inputs, after):
    return (lambda *refs: kernel(*refs[:inputs], *refs[inputs + len(after) :])), [pl.BlockSpec(memory_space=pl.ANY)] * len(after)


def params():
    return pltpu.CompilerParams(vmem_limit_bytes=VMEM_LIMIT, dimension_semantics=("arbitrary",))


def cost(matmuls, m, k, n, nbytes, exps=0):
    return pl.CostEstimate(flops=2 * matmuls * m * k * n, bytes_accessed=nbytes, transcendentals=exps)


def dot(a, b):
    return jnp.dot(a, b, preferred_element_type=F32)


def dot_nt(a, b):
    return lax.dot_general(a, b, (((1,), (1,)), ((), ())), preferred_element_type=F32)


def scale_of(wide):
    return lax.rsqrt(jnp.mean(wide * wide, -1, keepdims=True) + 1e-6)


def normed(h):
    wide = h.astype(F32)
    return (wide * scale_of(wide)).astype(BF16)


FEW = 2
WIDE = 2 * COLS


def forward_kernel(
    h_ref, wg_ref, wu_ref, wd_ref,
    wg0_ref, wu0_ref, wd0_ref, wg1_ref, wu1_ref, wd1_ref, hidden_ref, gate_ref, out_ref,
    a_ref, wg_all, wu_all, wd_all, own_g, own_u, own_d, land_g, land_u, land_d,
    hidden_out, gate_out, hidden_in, h_in, h_out,
    send, recv, send_b, recv_b, send_own, recv_own, local, keep, load, store,
):
    r, s = lax.axis_index("r"), lax.axis_index("s")
    sibling, across = s + 1 - 2 * lax.rem(s, 2), lax.rem(s + 2, 4)
    m, d = h_ref.shape
    f = wg_all.shape[1]
    steps = f // COLS
    blocks = 1 + (f - COLS) // WIDE

    def remote(src, dst, sends, recvs, where):
        return pltpu.make_async_remote_copy(
            src_ref=src, dst_ref=dst, send_sem=sends, recv_sem=recvs, device_id=where, device_id_type=pl.DeviceIdType.MESH
        )

    def target(kind):
        return {"r": 1 - r} if kind == 3 else {"s": across} if kind == 1 else {"s": sibling}

    def place(kind, size, row, rows):
        owner, which = (s, r) if kind == 1 else (across, r if kind < 4 else 1 - r)
        return pl.ds(owner * size + which * (size // 2) + row, rows)

    firsts = (wg_all, wu_all)

    def fine(kind, which, block):
        every = firsts[which]
        size = d // 4
        if isinstance(block, int) and block == 0:
            at = pl.ds(0, COLS)
        else:
            at = pl.ds(pl.multiple_of(COLS + (block - 1) * WIDE, COLS), WIDE)
        rows = pl.ds(s * size, size) if kind == 0 else place(kind, size, 0, size // 2)
        ref = every.at[rows, at]
        return remote(ref, ref, send.at[block, which, kind], recv.at[block, which, kind], target(kind))

    behind = (
        (wd_all, None, None, f // 4),
        (wg1_ref, own_g, land_g, d // 4),
        (wu1_ref, own_u, land_u, d // 4),
        (wd1_ref, own_d, land_d, f // 4),
    )

    def coarse(kind, which, piece):
        every, own, land, size = behind[which]
        rows = size // 2 // FEW
        row = piece * rows
        sems = send_b.at[which, piece, kind - 1], recv_b.at[which, piece, kind - 1]
        there = every.at[place(kind, size, row, rows)]
        if land is None:
            src = dst = there
        elif kind == 1:
            src, dst = own.at[pl.ds(r * (size // 2) + row, rows)], land.at[0, pl.ds(row, rows)]
        elif kind == 3:
            src, dst = land.at[0, pl.ds(row, rows)], land.at[1, pl.ds(row, rows)]
        else:
            src, dst = land.at[kind // 2 - 1, pl.ds(row, rows)], there
        return remote(src, dst, *sems, target(kind))

    def coarse_own(which):
        every, own, _, size = behind[which]
        there = every.at[pl.ds(s * size, size)]
        return remote(there if own is None else own, there, send_own.at[which], recv_own.at[which], target(0))

    def kept(which, piece, slot):
        every, _, land, size = behind[which]
        rows = size // 2 // FEW
        return pltpu.make_async_copy(
            land.at[slot, pl.ds(piece * rows, rows)],
            every.at[place(2 + 2 * slot, size, piece * rows, rows)],
            keep.at[which, piece, slot],
        )

    def kept_own(which):
        every, own, _, size = behind[which]
        return pltpu.make_async_copy(own, every.at[pl.ds(s * size, size)], keep.at[which, FEW, 0])

    loads = [
        pltpu.make_async_copy(wg_ref.at[0], wg_all.at[pl.ds(s * (d // 4), d // 4)], local.at[0]),
        pltpu.make_async_copy(wu_ref.at[0], wu_all.at[pl.ds(s * (d // 4), d // 4)], local.at[1]),
        pltpu.make_async_copy(wd_ref.at[0], wd_all.at[pl.ds(s * (f // 4), f // 4)], local.at[2]),
        pltpu.make_async_copy(wg_ref.at[1], own_g, local.at[3]),
        pltpu.make_async_copy(wu_ref.at[1], own_u, local.at[4]),
        pltpu.make_async_copy(wd_ref.at[1], own_d, local.at[5]),
    ]
    load_h = pltpu.make_async_copy(h_ref, a_ref, load.at[0])
    loads[0].start()
    loads[1].start()
    load_h.start()
    for copy in loads[2:]:
        copy.start()

    for which in range(2):
        loads[which].wait()
        fine(1, which, 0).start()
        fine(0, which, 0).start()

    def first_sends(block, carry):
        for kind in (1, 0):
            for which in range(2):
                fine(kind, which, block).start()
        return carry

    lax.fori_loop(1, blocks, first_sends, 0)

    def send_on(block):
        for which in range(2):
            fine(1, which, block).wait_recv()
            fine(3, which, block).start()
            fine(2, which, block).start()

    def send_last(block):
        for which in range(2):
            fine(3, which, block).wait_recv()
            fine(4, which, block).start()

    def arrived(block):
        for which in range(2):
            for kind in (0, 2, 4):
                fine(kind, which, block).wait_recv()

    load_h.wait()
    half = m // 2
    for row in range(0, half, ROWS):
        a_ref[row : row + ROWS, :] = normed(a_ref[row : row + ROWS, :])
    send_on(0)
    for row in range(half, m, ROWS):
        a_ref[row : row + ROWS, :] = normed(a_ref[row : row + ROWS, :])
    send_last(0)
    send_on(1)
    arrived(0)

    def out_copies(n, part):
        at = pl.ds(pl.multiple_of(n * COLS, COLS), COLS)
        rows = pl.ds(part * half, half)
        return (
            pltpu.make_async_copy(hidden_out.at[part], hidden_ref.at[rows, at], store.at[0, part]),
            pltpu.make_async_copy(gate_out.at[part], gate_ref.at[rows, at], store.at[1, part]),
        )

    def coarse_on(number):
        which, piece = number // FEW, number % FEW
        coarse(1, which, piece).wait_recv()
        coarse(3, which, piece).start()
        coarse(2, which, piece).start()
        if which:
            kept(which, piece, 0).start()

    def coarse_last(number):
        which, piece = number // FEW, number % FEW
        coarse(3, which, piece).wait_recv()
        coarse(4, which, piece).start()
        if which:
            kept(which, piece, 1).start()

    def begin(which):
        loads[2 + which].wait()
        for piece in range(FEW):
            coarse(1, which, piece).start()
        coarse_own(which).start()
        if which:
            kept_own(which).start()

    def at_steps(index, table, action):
        for when, number in table:
            @pl.when(index == when)
            def _(number=number):
                action(number)

    def step(n, carry):
        @pl.when((n >= 1) & (n < blocks - 1))
        def _():
            send_on(n + 1)

        at_steps(n, ((1, 0), (2, 1), (4, 2), (6, 3)), begin)
        at_steps(n, ((5, 0), (7, 1), (8, 2), (10, 3)), coarse_on)
        at_steps(n, ((8, 0), (9, 1)), coarse_last)

        @pl.when(lax.rem(n, 2) == 1)
        def _():
            arrived((n + 1) // 2)

        at = pl.ds(pl.multiple_of(n * COLS, COLS), COLS)
        for part in range(2):
            @pl.when(n >= 1)
            def _(part=part):
                for copy in out_copies(n - 1, part):
                    copy.wait()

            for row in range(0, half, 1024):
                rows = slice(part * half + row, part * half + row + 1024)
                gate = dot(a_ref[rows, :], wg_all[:, at])
                up = dot(a_ref[rows, :], wu_all[:, at])
                gate_out[part, row : row + 1024, :] = gate
                hidden_out[part, row : row + 1024, :] = (gate * jax.nn.sigmoid(gate) * up).astype(BF16)
            for copy in out_copies(n, part):
                copy.start()

        @pl.when((lax.rem(n, 2) == 0) & (n + 1 < steps))
        def _():
            send_last(n // 2 + 1)
        return carry

    lax.fori_loop(0, steps, step, 0)

    def tile_loads(i):
        slot = lax.rem(i, 2)
        rows = pl.ds(pl.multiple_of(i * ROWS, ROWS), ROWS)
        return (
            pltpu.make_async_copy(hidden_ref.at[rows], hidden_in.at[slot], load.at[slot]),
            pltpu.make_async_copy(h_ref.at[rows], h_in.at[slot], load.at[2 + slot]),
        )

    def tile_store(i):
        slot = lax.rem(i, 2)
        rows = pl.ds(pl.multiple_of(i * ROWS, ROWS), ROWS)
        return pltpu.make_async_copy(h_out.at[slot], out_ref.at[rows], store.at[2, slot])

    saves = [
        pltpu.make_async_copy(every, full, local.at[which])
        for which, (every, full) in enumerate(((wg_all, wg0_ref), (wu_all, wu0_ref), (wd_all, wd0_ref)))
    ]
    saves[0].start()
    saves[1].start()
    for part in range(2):
        for copy in out_copies(steps - 1, part):
            copy.wait()
    for copy in tile_loads(0):
        copy.start()
    coarse_own(0).wait_recv()
    for piece in range(FEW):
        coarse(2, 0, piece).wait_recv()
        coarse(4, 0, piece).wait_recv()
    saves[2].start()
    tile_count = m // ROWS

    def tile(i, carry):
        @pl.when(i + 1 < tile_count)
        def _():
            for copy in tile_loads(i + 1):
                copy.start()

        @pl.when(i >= 2)
        def _():
            tile_store(i - 2).wait()

        at_steps(i, ((0, 4), (2, 5), (4, 6), (6, 7)), coarse_on)
        at_steps(i, ((0, 2), (2, 3), (4, 4), (6, 5)), coarse_last)
        for copy in tile_loads(i):
            copy.wait()
        slot = lax.rem(i, 2)
        for c in range(d // COLS):
            at = slice(c * COLS, (c + 1) * COLS)
            h_out[slot, :, at] = h_in[slot, :, at] + dot(hidden_in[slot], wd_all[:, at]).astype(BF16)
        tile_store(i).start()
        return carry

    lax.fori_loop(0, tile_count, tile, 0)
    coarse_last(6)
    coarse_last(7)
    for i in (tile_count - 2, tile_count - 1):
        tile_store(i).wait()
    for save in saves:
        save.wait()
    for which in range(1, 4):
        kept_own(which).wait()
        coarse_own(which).wait_recv()
        for piece in range(FEW):
            kept(which, piece, 0).wait()
            kept(which, piece, 1).wait()
            coarse(2, which, piece).wait_recv()
            coarse(4, which, piece).wait_recv()
    for which in range(4):
        coarse_own(which).wait_send()
        for piece in range(FEW):
            for kind in range(1, 5):
                coarse(kind, which, piece).wait_send()

    def sent(block):
        for which in range(2):
            for kind in range(5):
                fine(kind, which, block).wait_send()

    sent(0)
    lax.fori_loop(1, blocks, lambda block, carry: (sent(block), carry)[1], 0)


def forward(h, w_gate, w_up, w_down):
    m, d = h.shape
    f = w_gate.shape[2]
    blocks = 1 + (f - COLS) // WIDE
    any_spec = pl.BlockSpec(memory_space=pl.ANY)
    up_shape, down_shape = jax.ShapeDtypeStruct((d, f), BF16), jax.ShapeDtypeStruct((f, d), BF16)
    dma = pltpu.SemaphoreType.DMA
    return pl.pallas_call(
        forward_kernel,
        in_specs=[any_spec] * 4,
        out_specs=[any_spec] * 9,
        out_shape=[
            up_shape, up_shape, down_shape, up_shape, up_shape, down_shape,
            jax.ShapeDtypeStruct((m, f), BF16),
            jax.ShapeDtypeStruct((m, f), F32),
            jax.ShapeDtypeStruct((m, d), BF16),
        ],
        scratch_shapes=[
            pltpu.VMEM((m, d), BF16),
            pltpu.VMEM((d, f), BF16),
            pltpu.VMEM((d, f), BF16),
            pltpu.VMEM((f, d), BF16),
            pltpu.VMEM((d // 4, f), BF16),
            pltpu.VMEM((d // 4, f), BF16),
            pltpu.VMEM((f // 4, d), BF16),
            pltpu.VMEM((2, d // 8, f), BF16),
            pltpu.VMEM((2, d // 8, f), BF16),
            pltpu.VMEM((2, f // 8, d), BF16),
            pltpu.VMEM((2, m // 2, COLS), BF16),
            pltpu.VMEM((2, m // 2, COLS), F32),
            pltpu.VMEM((2, ROWS, f), BF16),
            pltpu.VMEM((2, ROWS, d), BF16),
            pltpu.VMEM((2, ROWS, d), BF16),
            dma((blocks, 2, 5)), dma((blocks, 2, 5)),
            dma((4, FEW, 4)), dma((4, FEW, 4)),
            dma((4,)), dma((4,)), dma((6,)), dma((4, FEW + 1, 2)), dma((4,)), dma((3, 2)),
        ],
        compiler_params=pltpu.CompilerParams(vmem_limit_bytes=VMEM_LIMIT, has_side_effects=True),
        cost_estimate=cost(3, m, d, f, 4 * m * d + 24 * d * f + 8 * m * f, m * f),
        name="forward",
    )(h, w_gate, w_up, w_down)


def inner_kernel(kept, *refs):
    if kept:
        h_ref, g_ref, gate_ref, wu_ref, wd_ref, a_t_ref, hidden_t_ref, dgate_ref, dup_ref, a_ref = refs
    else:
        h_ref, g_ref, wg_ref, wu_ref, wd_ref, a_t_ref, hidden_t_ref, dgate_ref, dup_ref, a_ref = refs
    a = normed(h_ref[...])
    a_ref[...] = a
    a_t_ref[...] = a.T
    for c in range(wu_ref.shape[1] // COLS):
        at = slice(c * COLS, (c + 1) * COLS)
        gate = gate_ref[:, at] if kept else dot(a_ref[...], wg_ref[:, at])
        up = dot(a_ref[...], wu_ref[:, at])
        dhidden = dot_nt(g_ref[...], wd_ref[at, :]).astype(BF16).astype(F32)
        sig = jax.nn.sigmoid(gate)
        silu = gate * sig
        hidden_t_ref[at, :] = (silu * up).astype(BF16).T
        dup_ref[:, at] = (dhidden * silu).astype(BF16)
        dgate_ref[:, at] = (dhidden * up * (sig + silu * (1.0 - sig))).astype(BF16)


def inner_of(h, g, gate_or_wg, wu, wd, kept, after=()):
    m, d = h.shape
    f = wu.shape[1]
    kernel, extra = ordered(functools.partial(inner_kernel, kept), 5, after)
    return pl.pallas_call(
        kernel,
        grid=(m // ROWS,),
        in_specs=[
            tiles(ROWS, d),
            tiles(ROWS, d),
            tiles(ROWS, f) if kept else whole((d, f)),
            whole((d, f)),
            whole((f, d)),
            *extra,
        ],
        out_specs=[columns(d, ROWS), columns(f, ROWS), tiles(ROWS, f), tiles(ROWS, f)],
        out_shape=[
            jax.ShapeDtypeStruct((d, m), BF16),
            jax.ShapeDtypeStruct((f, m), BF16),
            jax.ShapeDtypeStruct((m, f), BF16),
            jax.ShapeDtypeStruct((m, f), BF16),
        ],
        scratch_shapes=[pltpu.VMEM((ROWS, d), BF16)],
        compiler_params=params(),
        cost_estimate=cost(2 if kept else 3, m, d, f, 6 * m * d + 6 * d * f + (10 if kept else 6) * m * f, m * f),
        name="inner_kept" if kept else "inner",
    )(h, g, gate_or_wg, wu, wd, *after)


def outer_kernel(dgate_ref, dup_ref, wg_ref, wu_ref, h_ref, g_ref, out_ref, da_ref):
    for c in range(wg_ref.shape[0] // COLS):
        at = slice(c * COLS, (c + 1) * COLS)
        one = dot_nt(dgate_ref[...], wg_ref[at, :]).astype(BF16)
        two = dot_nt(dup_ref[...], wu_ref[at, :]).astype(BF16)
        da_ref[:, at] = one + two
    wide = h_ref[...].astype(F32)
    da = da_ref[...].astype(F32)
    scale = scale_of(wide)
    along = jnp.mean(da * wide, -1, keepdims=True)
    out_ref[...] = g_ref[...] + (scale * (da - wide * (along * scale * scale))).astype(BF16)


def outer_of(dgate, dup, wg, wu, h, g, after=()):
    m, d = h.shape
    f = wg.shape[1]
    kernel, extra = ordered(outer_kernel, 6, after)
    return pl.pallas_call(
        kernel,
        grid=(m // ROWS,),
        in_specs=[tiles(ROWS, f), tiles(ROWS, f), whole((d, f)), whole((d, f)), tiles(ROWS, d), tiles(ROWS, d), *extra],
        out_specs=tiles(ROWS, d),
        out_shape=jax.ShapeDtypeStruct((m, d), BF16),
        scratch_shapes=[pltpu.VMEM((ROWS, d), BF16)],
        compiler_params=params(),
        cost_estimate=cost(2, m, d, f, 6 * m * d + 4 * d * f + 4 * m * f),
        name="outer",
    )(dgate, dup, wg, wu, h, g, *after)


def by_columns_kernel(a_ref, b_ref, out_ref):
    out_ref[...] = dot(a_ref[...], b_ref[...]).astype(BF16)


def by_columns(a_t, b, after=()):
    d, m = a_t.shape
    f = b.shape[1]
    kernel, extra = ordered(by_columns_kernel, 2, after)
    return pl.pallas_call(
        kernel,
        grid=(f // COLS,),
        in_specs=[whole((d, m)), columns(m, COLS), *extra],
        out_specs=columns(d, COLS),
        out_shape=jax.ShapeDtypeStruct((d, f), BF16),
        compiler_params=params(),
        cost_estimate=cost(1, m, d, f, 2 * m * d + 2 * d * f + 2 * m * f),
        name="by_columns",
    )(a_t, b, *after)


def by_rows_kernel(a_ref, b_ref, out_ref):
    for c in range(b_ref.shape[1] // COLS):
        at = slice(c * COLS, (c + 1) * COLS)
        out_ref[:, at] = dot(a_ref[...], b_ref[:, at]).astype(BF16)


def by_rows(a_t, b, after=()):
    f, m = a_t.shape
    d = b.shape[1]
    rows = f // 4
    kernel, extra = ordered(by_rows_kernel, 2, after)
    return pl.pallas_call(
        kernel,
        grid=(4,),
        in_specs=[tiles(rows, m), whole((m, d)), *extra],
        out_specs=tiles(rows, d),
        out_shape=jax.ShapeDtypeStruct((f, d), BF16),
        compiler_params=params(),
        cost_estimate=cost(1, m, d, f, 2 * m * d + 2 * d * f + 2 * m * f),
        name="by_rows",
    )(a_t, b, *after)


def solution(mesh):
    groups = mesh.shape["r"]
    other = [(i, (i + 1) % groups) for i in range(groups)]

    def scattered(term):
        return lax.psum_scatter(term, "s", scatter_dimension=0, tiled=True)

    def swapped(mine):
        return lax.ppermute(mine, "r", other)

    def step(x, dy, w_gate, w_up, w_down):
        h0, g2 = x[0], dy[0]
        wg0, wu0, wd0, wg1, wu1, wd1, _, gate, h1 = forward(h0, w_gate, w_up, w_down)

        a_t, hidden_t, dgate, dup = inner_of(h1, g2, wg1, wu1, wd1, False)
        by_down = by_rows(hidden_t, g2)
        down1 = scattered(by_down)
        by_gate = by_columns(a_t, dgate, (by_down,))
        gate1 = scattered(by_gate)
        by_up = by_columns(a_t, dup, (by_gate,))
        up1 = scattered(by_up)
        g1 = outer_of(dgate, dup, wg1, wu1, h1, g2, (by_up, down1))
        down1_r = swapped(down1)

        a_t, hidden_t, dgate, dup = inner_of(h0, g1, gate, wu0, wd0, True, (gate1, down1_r))
        gate1_r = swapped(gate1)
        by_down = by_rows(hidden_t, g1, (up1, gate1_r))
        down0 = scattered(by_down)
        up1_r = swapped(up1)
        by_gate = by_columns(a_t, dgate, (by_down,))
        gate0 = scattered(by_gate)
        by_up = by_columns(a_t, dup, (by_gate,))
        up0 = scattered(by_up)
        g0 = outer_of(dgate, dup, wg0, wu0, h0, g1, (by_up, down0))
        down0_r = swapped(down0)
        g0, gate0, up0 = lax.optimization_barrier((g0, gate0, up0))
        gate0_r, up0_r = swapped(gate0), swapped(up0)

        def both(*pairs):
            return jnp.stack([a.astype(F32) + b.astype(F32) for a, b in pairs]).astype(BF16)

        return (
            g0[None],
            both((gate0, gate0_r), (gate1, gate1_r)),
            both((up0, up0_r), (up1, up1_r)),
            both((down0, down0_r), (down1, down1_r)),
        )

    states, cut = P(("rep", "r", "s"), None, None), P(None, "s", None)
    return jax.shard_map(
        step,
        mesh=mesh,
        in_specs=(states, states) + (cut,) * 3,
        out_specs=(states,) + (P("rep", "s", None),) * 3,
        check_vma=False,
    )
```

```python
import functools

import jax
import jax.numpy as jnp
from jax import lax
from jax.experimental import pallas as pl
from jax.experimental.pallas import tpu as pltpu
from jax.sharding import PartitionSpec as P


F32, BF16 = jnp.float32, jnp.bfloat16
ROWS = 512
COLS = 256
VMEM_LIMIT = 60 * 1024 * 1024


def whole(shape):
    return pl.BlockSpec(shape, lambda i: (0,) * len(shape), pipeline_mode=pl.Buffered(1))


def tiles(rows, width):
    return pl.BlockSpec((rows, width), lambda i: (i, 0))


def columns(height, cols):
    return pl.BlockSpec((height, cols), lambda i: (0, i))


def ordered(kernel, inputs, after):
    return (lambda *refs: kernel(*refs[:inputs], *refs[inputs + len(after) :])), [pl.BlockSpec(memory_space=pl.ANY)] * len(after)


def params(remote=False):
    return pltpu.CompilerParams(vmem_limit_bytes=VMEM_LIMIT, dimension_semantics=("arbitrary",), has_side_effects=remote)


def cost(matmuls, m, k, n, nbytes, exps=0):
    return pl.CostEstimate(flops=2 * matmuls * m * k * n, bytes_accessed=nbytes, transcendentals=exps)


def dot(a, b):
    return jnp.dot(a, b, preferred_element_type=F32)


def dot_nt(a, b):
    return lax.dot_general(a, b, (((1,), (1,)), ((), ())), preferred_element_type=F32)


def scale_of(wide):
    return lax.rsqrt(jnp.mean(wide * wide, -1, keepdims=True) + 1e-6)


def normed(h):
    wide = h.astype(F32)
    return (wide * scale_of(wide)).astype(BF16)


FEW = 2
WIDE = 2 * COLS


def forward_kernel(
    h_ref, wg_ref, wu_ref, wd_ref,
    wg0_ref, wu0_ref, wd0_ref, wg1_ref, wu1_ref, wd1_ref, hidden_ref, gate_ref, out_ref,
    a_ref, wg_all, wu_all, wd_all, own_g, own_u, own_d, land_g, land_u, land_d,
    hidden_out, gate_out, hidden_in, h_in, h_out,
    send, recv, send_b, recv_b, send_own, recv_own, local, keep, load, store,
):
    r, s = lax.axis_index("r"), lax.axis_index("s")
    sibling, across = s + 1 - 2 * lax.rem(s, 2), lax.rem(s + 2, 4)
    m, d = h_ref.shape
    f = wg_all.shape[1]
    steps = f // COLS
    blocks = 1 + (f - COLS) // WIDE

    def remote(src, dst, sends, recvs, where):
        return pltpu.make_async_remote_copy(
            src_ref=src, dst_ref=dst, send_sem=sends, recv_sem=recvs, device_id=where, device_id_type=pl.DeviceIdType.MESH
        )

    def target(kind):
        return {"r": 1 - r} if kind == 3 else {"s": across} if kind == 1 else {"s": sibling}

    def place(kind, size, row, rows):
        owner, which = (s, r) if kind == 1 else (across, r if kind < 4 else 1 - r)
        return pl.ds(owner * size + which * (size // 2) + row, rows)

    firsts = (wg_all, wu_all)

    def fine(kind, which, block):
        every = firsts[which]
        size = d // 4
        if isinstance(block, int) and block == 0:
            at = pl.ds(0, COLS)
        else:
            at = pl.ds(pl.multiple_of(COLS + (block - 1) * WIDE, COLS), WIDE)
        rows = pl.ds(s * size, size) if kind == 0 else place(kind, size, 0, size // 2)
        ref = every.at[rows, at]
        return remote(ref, ref, send.at[block, which, kind], recv.at[block, which, kind], target(kind))

    behind = (
        (wd_all, None, None, f // 4),
        (wg1_ref, own_g, land_g, d // 4),
        (wu1_ref, own_u, land_u, d // 4),
        (wd1_ref, own_d, land_d, f // 4),
    )

    def coarse(kind, which, piece):
        every, own, land, size = behind[which]
        rows = size // 2 // FEW
        row = piece * rows
        sems = send_b.at[which, piece, kind - 1], recv_b.at[which, piece, kind - 1]
        there = every.at[place(kind, size, row, rows)]
        if land is None:
            src = dst = there
        elif kind == 1:
            src, dst = own.at[pl.ds(r * (size // 2) + row, rows)], land.at[0, pl.ds(row, rows)]
        elif kind == 3:
            src, dst = land.at[0, pl.ds(row, rows)], land.at[1, pl.ds(row, rows)]
        else:
            src, dst = land.at[kind // 2 - 1, pl.ds(row, rows)], there
        return remote(src, dst, *sems, target(kind))

    def coarse_own(which):
        every, own, _, size = behind[which]
        there = every.at[pl.ds(s * size, size)]
        return remote(there if own is None else own, there, send_own.at[which], recv_own.at[which], target(0))

    def kept(which, piece, slot):
        every, _, land, size = behind[which]
        rows = size // 2 // FEW
        return pltpu.make_async_copy(
            land.at[slot, pl.ds(piece * rows, rows)],
            every.at[place(2 + 2 * slot, size, piece * rows, rows)],
            keep.at[which, piece, slot],
        )

    def kept_own(which):
        every, own, _, size = behind[which]
        return pltpu.make_async_copy(own, every.at[pl.ds(s * size, size)], keep.at[which, FEW, 0])

    loads = [
        pltpu.make_async_copy(wg_ref.at[0], wg_all.at[pl.ds(s * (d // 4), d // 4)], local.at[0]),
        pltpu.make_async_copy(wu_ref.at[0], wu_all.at[pl.ds(s * (d // 4), d // 4)], local.at[1]),
        pltpu.make_async_copy(wd_ref.at[0], wd_all.at[pl.ds(s * (f // 4), f // 4)], local.at[2]),
        pltpu.make_async_copy(wg_ref.at[1], own_g, local.at[3]),
        pltpu.make_async_copy(wu_ref.at[1], own_u, local.at[4]),
        pltpu.make_async_copy(wd_ref.at[1], own_d, local.at[5]),
    ]
    load_h = pltpu.make_async_copy(h_ref, a_ref, load.at[0])
    loads[0].start()
    loads[1].start()
    load_h.start()
    for copy in loads[2:]:
        copy.start()

    for which in range(2):
        loads[which].wait()
        fine(1, which, 0).start()
        fine(0, which, 0).start()

    def first_sends(block, carry):
        for kind in (1, 0):
            for which in range(2):
                fine(kind, which, block).start()
        return carry

    lax.fori_loop(1, blocks, first_sends, 0)

    def send_on(block):
        for which in range(2):
            fine(1, which, block).wait_recv()
            fine(3, which, block).start()
            fine(2, which, block).start()

    def send_last(block):
        for which in range(2):
            fine(3, which, block).wait_recv()
            fine(4, which, block).start()

    def arrived(block):
        for which in range(2):
            for kind in (0, 2, 4):
                fine(kind, which, block).wait_recv()

    load_h.wait()
    half = m // 2
    for row in range(0, half, ROWS):
        a_ref[row : row + ROWS, :] = normed(a_ref[row : row + ROWS, :])
    send_on(0)
    for row in range(half, m, ROWS):
        a_ref[row : row + ROWS, :] = normed(a_ref[row : row + ROWS, :])
    send_last(0)
    send_on(1)
    arrived(0)

    def out_copies(n, part):
        at = pl.ds(pl.multiple_of(n * COLS, COLS), COLS)
        rows = pl.ds(part * half, half)
        return (
            pltpu.make_async_copy(hidden_out.at[part], hidden_ref.at[rows, at], store.at[0, part]),
            pltpu.make_async_copy(gate_out.at[part], gate_ref.at[rows, at], store.at[1, part]),
        )

    def coarse_on(number):
        which, piece = number // FEW, number % FEW
        coarse(1, which, piece).wait_recv()
        coarse(3, which, piece).start()
        coarse(2, which, piece).start()
        if which:
            kept(which, piece, 0).start()

    def coarse_last(number):
        which, piece = number // FEW, number % FEW
        coarse(3, which, piece).wait_recv()
        coarse(4, which, piece).start()
        if which:
            kept(which, piece, 1).start()

    def begin(which):
        loads[2 + which].wait()
        for piece in range(FEW):
            coarse(1, which, piece).start()
        coarse_own(which).start()
        if which:
            kept_own(which).start()

    def at_steps(index, table, action):
        for when, number in table:
            @pl.when(index == when)
            def _(number=number):
                action(number)

    def step(n, carry):
        @pl.when((n >= 1) & (n < blocks - 1))
        def _():
            send_on(n + 1)

        at_steps(n, ((1, 0), (2, 1), (4, 2), (6, 3)), begin)
        at_steps(n, ((5, 0), (7, 1), (8, 2), (10, 3)), coarse_on)
        at_steps(n, ((8, 0), (9, 1)), coarse_last)

        @pl.when(lax.rem(n, 2) == 1)
        def _():
            arrived((n + 1) // 2)

        at = pl.ds(pl.multiple_of(n * COLS, COLS), COLS)
        for part in range(2):
            @pl.when(n >= 1)
            def _(part=part):
                for copy in out_copies(n - 1, part):
                    copy.wait()

            for row in range(0, half, 1024):
                rows = slice(part * half + row, part * half + row + 1024)
                gate = dot(a_ref[rows, :], wg_all[:, at])
                up = dot(a_ref[rows, :], wu_all[:, at])
                gate_out[part, row : row + 1024, :] = gate
                hidden_out[part, row : row + 1024, :] = (gate * jax.nn.sigmoid(gate) * up).astype(BF16)
            for copy in out_copies(n, part):
                copy.start()

        @pl.when((lax.rem(n, 2) == 0) & (n + 1 < steps))
        def _():
            send_last(n // 2 + 1)

        return carry

    lax.fori_loop(0, steps, step, 0)

    def tile_loads(i):
        slot = lax.rem(i, 2)
        rows = pl.ds(pl.multiple_of(i * ROWS, ROWS), ROWS)
        return (
            pltpu.make_async_copy(hidden_ref.at[rows], hidden_in.at[slot], load.at[slot]),
            pltpu.make_async_copy(h_ref.at[rows], h_in.at[slot], load.at[2 + slot]),
        )

    def tile_store(i):
        slot = lax.rem(i, 2)
        rows = pl.ds(pl.multiple_of(i * ROWS, ROWS), ROWS)
        return pltpu.make_async_copy(h_out.at[slot], out_ref.at[rows], store.at[2, slot])

    saves = [
        pltpu.make_async_copy(every, full, local.at[which])
        for which, (every, full) in enumerate(((wg_all, wg0_ref), (wu_all, wu0_ref), (wd_all, wd0_ref)))
    ]
    saves[0].start()
    saves[1].start()
    for part in range(2):
        for copy in out_copies(steps - 1, part):
            copy.wait()
    for copy in tile_loads(0):
        copy.start()
    coarse_own(0).wait_recv()
    for piece in range(FEW):
        coarse(2, 0, piece).wait_recv()
        coarse(4, 0, piece).wait_recv()
    saves[2].start()
    tile_count = m // ROWS

    def tile(i, carry):
        @pl.when(i + 1 < tile_count)
        def _():
            for copy in tile_loads(i + 1):
                copy.start()

        @pl.when(i >= 2)
        def _():
            tile_store(i - 2).wait()

        at_steps(i, ((0, 4), (2, 5), (4, 6), (6, 7)), coarse_on)
        at_steps(i, ((0, 2), (2, 3), (4, 4), (6, 5)), coarse_last)
        for copy in tile_loads(i):
            copy.wait()
        slot = lax.rem(i, 2)
        for c in range(d // COLS):
            at = slice(c * COLS, (c + 1) * COLS)
            h_out[slot, :, at] = h_in[slot, :, at] + dot(hidden_in[slot], wd_all[:, at]).astype(BF16)
        tile_store(i).start()
        return carry

    lax.fori_loop(0, tile_count, tile, 0)
    coarse_last(6)
    coarse_last(7)
    for i in (tile_count - 2, tile_count - 1):
        tile_store(i).wait()
    for save in saves:
        save.wait()
    for which in range(1, 4):
        kept_own(which).wait()
        coarse_own(which).wait_recv()
        for piece in range(FEW):
            kept(which, piece, 0).wait()
            kept(which, piece, 1).wait()
            coarse(2, which, piece).wait_recv()
            coarse(4, which, piece).wait_recv()
    for which in range(4):
        coarse_own(which).wait_send()
        for piece in range(FEW):
            for kind in range(1, 5):
                coarse(kind, which, piece).wait_send()

    def sent(block):
        for which in range(2):
            for kind in range(5):
                fine(kind, which, block).wait_send()

    sent(0)
    lax.fori_loop(1, blocks, lambda block, carry: (sent(block), carry)[1], 0)


def forward(h, w_gate, w_up, w_down):
    m, d = h.shape
    f = w_gate.shape[2]
    blocks = 1 + (f - COLS) // WIDE
    any_spec = pl.BlockSpec(memory_space=pl.ANY)
    up_shape, down_shape = jax.ShapeDtypeStruct((d, f), BF16), jax.ShapeDtypeStruct((f, d), BF16)
    dma = pltpu.SemaphoreType.DMA
    return pl.pallas_call(
        forward_kernel,
        in_specs=[any_spec] * 4,
        out_specs=[any_spec] * 9,
        out_shape=[
            up_shape, up_shape, down_shape, up_shape, up_shape, down_shape,
            jax.ShapeDtypeStruct((m, f), BF16),
            jax.ShapeDtypeStruct((m, f), F32),
            jax.ShapeDtypeStruct((m, d), BF16),
        ],
        scratch_shapes=[
            pltpu.VMEM((m, d), BF16),
            pltpu.VMEM((d, f), BF16),
            pltpu.VMEM((d, f), BF16),
            pltpu.VMEM((f, d), BF16),
            pltpu.VMEM((d // 4, f), BF16),
            pltpu.VMEM((d // 4, f), BF16),
            pltpu.VMEM((f // 4, d), BF16),
            pltpu.VMEM((2, d // 8, f), BF16),
            pltpu.VMEM((2, d // 8, f), BF16),
            pltpu.VMEM((2, f // 8, d), BF16),
            pltpu.VMEM((2, m // 2, COLS), BF16),
            pltpu.VMEM((2, m // 2, COLS), F32),
            pltpu.VMEM((2, ROWS, f), BF16),
            pltpu.VMEM((2, ROWS, d), BF16),
            pltpu.VMEM((2, ROWS, d), BF16),
            dma((blocks, 2, 5)), dma((blocks, 2, 5)),
            dma((4, FEW, 4)), dma((4, FEW, 4)),
            dma((4,)), dma((4,)), dma((6,)), dma((4, FEW + 1, 2)), dma((4,)), dma((3, 2)),
        ],
        compiler_params=pltpu.CompilerParams(vmem_limit_bytes=VMEM_LIMIT, has_side_effects=True),
        cost_estimate=cost(3, m, d, f, 4 * m * d + 24 * d * f + 8 * m * f, m * f),
        name="forward",
    )(h, w_gate, w_up, w_down)


PIECES = 8


def reducer_scratch(rows, f):
    block, dma = pltpu.VMEM((rows, f), BF16), pltpu.SemaphoreType.DMA
    pair = pltpu.VMEM((2, rows, f), BF16)
    return [pair, pair, block, block, block, block, block, dma((2, PIECES, 2)), dma((2, PIECES, 2)), dma((3,))]


class Reducer:
    def __init__(self, term, out, scratch, far_lag, last_lag):
        self.term, self.out = term, out
        self.own, self.sib, self.go, self.far, self.near, self.last, self.sum, self.first_sems, self.link_sems, self.local = scratch
        self.far_lag, self.last_lag = far_lag, last_lag
        self.r, self.s = lax.axis_index("r"), lax.axis_index("s")
        self.sibling, self.across = self.s + 1 - 2 * lax.rem(self.s, 2), lax.rem(self.s + 2, 4)
        self.rows = term.shape[0] // 4
        self.step = self.rows // PIECES

    def at(self, p):
        return pl.ds(p * self.step if isinstance(p, int) else pl.multiple_of(p * self.step, self.step), self.step)

    def remote(self, src, dst, send, recv, where):
        return pltpu.make_async_remote_copy(
            src_ref=src, dst_ref=dst, send_sem=send, recv_sem=recv, device_id=where, device_id_type=pl.DeviceIdType.MESH
        )

    def to_sibling(self, slot, p):
        shard = self.sibling if slot else lax.rem(self.sibling + 2, 4)
        return self.remote(
            self.term.at[pl.ds(shard * self.rows + p * self.step, self.step)],
            self.sib.at[slot, self.at(p)],
            self.first_sems.at[slot, p, 0],
            self.first_sems.at[slot, p, 1],
            {"s": self.sibling},
        )

    def to_across(self, p):
        return self.remote(self.go.at[self.at(p)], self.far.at[self.at(p)], self.link_sems.at[0, p, 0], self.link_sems.at[0, p, 1], {"s": self.across})

    def to_other(self, p):
        return self.remote(self.near.at[self.at(p)], self.last.at[self.at(p)], self.link_sems.at[1, p, 0], self.link_sems.at[1, p, 1], {"r": 1 - self.r})

    def load(self, slot):
        shard = self.s if slot else self.across
        return pltpu.make_async_copy(self.term.at[pl.ds(shard * self.rows, self.rows)], self.own.at[slot], self.local.at[slot])

    def begin(self):
        self.load(0).start()
        self.load(1).start()
        for slot in range(2):
            for p in range(PIECES):
                self.to_sibling(slot, p).start()
        self.load(0).wait()
        self.load(1).wait()

    def tick(self, t):
        def when(p, action):
            @pl.when((p >= 0) & (p < PIECES))
            def _():
                action(p)

        def wide(ref, p, *slot):
            return ref[(*slot, self.at(p))].astype(F32)

        def first(p):
            self.to_sibling(0, p).wait_recv()
            self.go[self.at(p)] = (wide(self.own, p, 0) + wide(self.sib, p, 0)).astype(BF16)

        def second(p):
            self.to_sibling(1, p).wait_recv()
            self.to_across(p).wait_recv()
            self.near[self.at(p)] = (wide(self.own, p, 1) + wide(self.sib, p, 1) + wide(self.far, p)).astype(BF16)

        def third(p):
            self.to_other(p).wait_recv()
            self.sum[self.at(p)] = (wide(self.near, p) + wide(self.last, p)).astype(BF16)

        when(t - 1, lambda p: self.to_across(p).start())
        when(t - self.far_lag - 1, lambda p: self.to_other(p).start())
        when(t, first)
        when(t - self.far_lag, second)
        when(t - self.last_lag, third)

    def finish(self, ticks):
        lax.fori_loop(ticks, PIECES + self.last_lag, lambda t, carry: (self.tick(t), carry)[1], 0)
        save = pltpu.make_async_copy(self.sum, self.out, self.local.at[2])
        save.start()
        for p in range(PIECES):
            self.to_sibling(0, p).wait_send()
            self.to_sibling(1, p).wait_send()
            self.to_across(p).wait_send()
            self.to_other(p).wait_send()
        save.wait()


def inner_kernel(kept, *refs):
    if kept:
        h_ref, g_ref, gate_ref, wu_ref, wd_ref, a_t_ref, hidden_t_ref, dgate_ref, dup_ref, a_ref = refs
    else:
        h_ref, g_ref, wg_ref, wu_ref, wd_ref, a_t_ref, hidden_t_ref, dgate_ref, dup_ref, a_ref = refs
    a = normed(h_ref[...])
    a_ref[...] = a
    a_t_ref[...] = a.T
    for c in range(wu_ref.shape[1] // COLS):
        at = slice(c * COLS, (c + 1) * COLS)
        gate = gate_ref[:, at] if kept else dot(a_ref[...], wg_ref[:, at])
        up = dot(a_ref[...], wu_ref[:, at])
        dhidden = dot_nt(g_ref[...], wd_ref[at, :]).astype(BF16).astype(F32)
        sig = jax.nn.sigmoid(gate)
        silu = gate * sig
        hidden_t_ref[at, :] = (silu * up).astype(BF16).T
        dup_ref[:, at] = (dhidden * silu).astype(BF16)
        dgate_ref[:, at] = (dhidden * up * (sig + silu * (1.0 - sig))).astype(BF16)


def inner_of(h, g, gate_or_wg, wu, wd, kept, after=()):
    m, d = h.shape
    f = wu.shape[1]
    kernel, extra = ordered(functools.partial(inner_kernel, kept), 5, after)
    return pl.pallas_call(
        kernel,
        grid=(m // ROWS,),
        in_specs=[
            tiles(ROWS, d),
            tiles(ROWS, d),
            tiles(ROWS, f) if kept else whole((d, f)),
            whole((d, f)),
            whole((f, d)),
            *extra,
        ],
        out_specs=[columns(d, ROWS), columns(f, ROWS), tiles(ROWS, f), tiles(ROWS, f)],
        out_shape=[
            jax.ShapeDtypeStruct((d, m), BF16),
            jax.ShapeDtypeStruct((f, m), BF16),
            jax.ShapeDtypeStruct((m, f), BF16),
            jax.ShapeDtypeStruct((m, f), BF16),
        ],
        scratch_shapes=[pltpu.VMEM((ROWS, d), BF16)],
        compiler_params=params(),
        cost_estimate=cost(2 if kept else 3, m, d, f, 6 * m * d + 6 * d * f + (10 if kept else 6) * m * f, m * f),
        name="inner_kept" if kept else "inner",
    )(h, g, gate_or_wg, wu, wd, *after)


def outer_kernel(carries, *refs):
    if carries:
        dgate_ref, dup_ref, wg_ref, wu_ref, h_ref, g_ref, term_ref, out_ref, sum_ref, da_ref, *scratch = refs
        reducer = Reducer(term_ref, sum_ref, scratch, 3, 6)
    else:
        dgate_ref, dup_ref, wg_ref, wu_ref, h_ref, g_ref, out_ref, da_ref = refs
    i, chunks = pl.program_id(0), wg_ref.shape[0] // COLS
    if carries:
        pl.when(i == 0)(reducer.begin)
    for c in range(chunks):
        if carries and c % (chunks // 2) == 0:
            reducer.tick(2 * i + c // (chunks // 2))
        at = slice(c * COLS, (c + 1) * COLS)
        one = dot_nt(dgate_ref[...], wg_ref[at, :]).astype(BF16)
        two = dot_nt(dup_ref[...], wu_ref[at, :]).astype(BF16)
        da_ref[:, at] = one + two
    wide = h_ref[...].astype(F32)
    da = da_ref[...].astype(F32)
    scale = scale_of(wide)
    along = jnp.mean(da * wide, -1, keepdims=True)
    out_ref[...] = g_ref[...] + (scale * (da - wide * (along * scale * scale))).astype(BF16)
    if carries:
        steps = pl.num_programs(0)
        pl.when(i == steps - 1)(lambda: reducer.finish(2 * steps))


def outer_of(dgate, dup, wg, wu, h, g, after=(), term=None):
    m, d = h.shape
    f = wg.shape[1]
    carries = [] if term is None else [term]
    any_spec = [pl.BlockSpec(memory_space=pl.ANY)] * len(carries)
    block = [jax.ShapeDtypeStruct((t.shape[0] // 4, t.shape[1]), BF16) for t in carries]
    kernel, extra = ordered(functools.partial(outer_kernel, bool(carries)), 6 + len(carries), after)
    out = pl.pallas_call(
        kernel,
        grid=(m // ROWS,),
        in_specs=[tiles(ROWS, f), tiles(ROWS, f), whole((d, f)), whole((d, f)), tiles(ROWS, d), tiles(ROWS, d), *any_spec, *extra],
        out_specs=[tiles(ROWS, d), *any_spec],
        out_shape=[jax.ShapeDtypeStruct((m, d), BF16), *block],
        scratch_shapes=[pltpu.VMEM((ROWS, d), BF16)] + [x for b in block for x in reducer_scratch(*b.shape)],
        compiler_params=params(bool(carries)),
        cost_estimate=cost(2, m, d, f, 6 * m * d + 4 * d * f + 4 * m * f),
        name="outer_reduce" if carries else "outer",
    )(dgate, dup, wg, wu, h, g, *carries, *after)
    return out if carries else out[0]


def by_columns_kernel(carries, *refs):
    if carries:
        a_ref, b_ref, term_ref, out_ref, sum_ref, *scratch = refs
        i, steps = pl.program_id(0), pl.num_programs(0)
        reducer = Reducer(term_ref, sum_ref, scratch, 4, 8)
        pl.when(i == 0)(reducer.begin)
        reducer.tick(i)
    else:
        a_ref, b_ref, out_ref = refs
    out_ref[...] = dot(a_ref[...], b_ref[...]).astype(BF16)
    if carries:
        pl.when(i == steps - 1)(lambda: reducer.finish(steps))


def by_columns(a_t, b, after=(), term=None):
    d, m = a_t.shape
    f = b.shape[1]
    carries = [] if term is None else [term]
    any_spec = [pl.BlockSpec(memory_space=pl.ANY)] * len(carries)
    block = [jax.ShapeDtypeStruct((t.shape[0] // 4, t.shape[1]), BF16) for t in carries]
    kernel, extra = ordered(functools.partial(by_columns_kernel, bool(carries)), 2 + len(carries), after)
    out = pl.pallas_call(
        kernel,
        grid=(f // COLS,),
        in_specs=[whole((d, m)), columns(m, COLS), *any_spec, *extra],
        out_specs=[columns(d, COLS), *any_spec],
        out_shape=[jax.ShapeDtypeStruct((d, f), BF16), *block],
        scratch_shapes=[x for b in block for x in reducer_scratch(*b.shape)],
        compiler_params=params(bool(carries)),
        cost_estimate=cost(1, m, d, f, 2 * m * d + 2 * d * f + 2 * m * f),
        name="by_columns_reduce" if carries else "by_columns",
    )(a_t, b, *carries, *after)
    return out if carries else out[0]


def by_rows_kernel(a_ref, b_ref, out_ref):
    for c in range(b_ref.shape[1] // COLS):
        at = slice(c * COLS, (c + 1) * COLS)
        out_ref[:, at] = dot(a_ref[...], b_ref[:, at]).astype(BF16)


def by_rows(a_t, b, after=()):
    f, m = a_t.shape
    d = b.shape[1]
    rows = f // 4
    kernel, extra = ordered(by_rows_kernel, 2, after)
    return pl.pallas_call(
        kernel,
        grid=(4,),
        in_specs=[tiles(rows, m), whole((m, d)), *extra],
        out_specs=tiles(rows, d),
        out_shape=jax.ShapeDtypeStruct((f, d), BF16),
        compiler_params=params(),
        cost_estimate=cost(1, m, d, f, 2 * m * d + 2 * d * f + 2 * m * f),
        name="by_rows",
    )(a_t, b, *after)


def solution(mesh):
    groups = mesh.shape["r"]
    other = [(i, (i + 1) % groups) for i in range(groups)]

    def scattered(term):
        return lax.psum_scatter(term, "s", scatter_dimension=0, tiled=True)

    def swapped(mine):
        return lax.ppermute(mine, "r", other)

    def step(x, dy, w_gate, w_up, w_down):
        h0, g2 = x[0], dy[0]
        wg0, wu0, wd0, wg1, wu1, wd1, _, gate, h1 = forward(h0, w_gate, w_up, w_down)

        a_t, hidden_t, dgate, dup = inner_of(h1, g2, wg1, wu1, wd1, False)
        by_down = by_rows(hidden_t, g2)
        down1 = scattered(by_down)
        by_gate = by_columns(a_t, dgate, (by_down,))
        gate1 = scattered(by_gate)
        by_up = by_columns(a_t, dup, (by_gate,))
        up1 = scattered(by_up)
        g1 = outer_of(dgate, dup, wg1, wu1, h1, g2, (by_up, down1))
        down1_r = swapped(down1)

        a_t, hidden_t, dgate, dup = inner_of(h0, g1, gate, wu0, wd0, True, (gate1, down1_r))
        gate1_r = swapped(gate1)
        by_down = by_rows(hidden_t, g1, (up1, gate1_r))
        down0 = scattered(by_down)
        up1_r = swapped(up1)
        by_gate = by_columns(a_t, dgate, (by_down,))
        by_up, gate0 = by_columns(a_t, dup, (), by_gate)
        sums = lax.optimization_barrier((gate0, gate1, gate1_r, up1, up1_r, down1, down1_r))
        gate0, gate1, gate1_r, up1, up1_r, down1, down1_r = sums
        g0, up0 = outer_of(dgate, dup, wg0, wu0, h0, g1, (down0,), by_up)
        down0_r = swapped(down0)

        def both(a, b):
            return (a.astype(F32) + b.astype(F32)).astype(BF16)

        return (
            g0[None],
            jnp.stack([gate0, both(gate1, gate1_r)]),
            jnp.stack([up0, both(up1, up1_r)]),
            jnp.stack([both(down0, down0_r), both(down1, down1_r)]),
        )

    states, cut = P(("rep", "r", "s"), None, None), P(None, "s", None)
    return jax.shard_map(
        step,
        mesh=mesh,
        in_specs=(states, states) + (cut,) * 3,
        out_specs=(states,) + (P("rep", "s", None),) * 3,
        check_vma=False,
    )
```
